32 devices in a mesh: seed: 2 (over core), dp: 4 (over y, x), tensor: 4 (over z).
Axes of the slice: x: 2, y: 2, z: 4, core: 2. Of those that a mesh axis runs over, the one named last changes fastest.
Arguments:
- hidden: bfloat16 [2, 64, 96, 2048], P('seed', 'dp', None, 'tensor'), may hold values from -24 to 24
- norm_gain: float32 [2, 2048], P('seed'), may hold values from 0.25 to 1.75
- lm_head: bfloat16 [2, 2048, 4096], P('seed', None, 'tensor'), may hold values from -3 to 3
- targets: int32 [64, 96], P('dp'), may hold values from 0 to 4095
- lengths: int32 [64], P('dp'), may hold values from 24 to 96
Outputs:
- token_scores: float32 [2, 64, 96], P('seed', 'dp')
- ensemble: float32 [64], P('dp')
- centered: float32 [64], P('dp')
The draws below stay inside these ranges and needn't reach their ends.
All inputs are finite; a program needn't handle non-finite values.
Results may differ from the reference program's by a relative error of at most 0.0003.
The reference program's roundings to bfloat16 on the way (of `normed`) count: a program that leaves them out, or rounds other values in their place, can miss the bound.
Values may be sent and summed in bfloat16 or wider, within the bound.
A program may use at most 128 MiB of HBM per device.

```python
import math
import jax
import jax.numpy as jnp
from jax import lax

D = 2048
VOCAB = 4096
SEQ = 96
EXAMPLES = 64
SEEDS = 2


plain_scale = 3.0


def shared_chosen(key):
    return jax.random.randint(jax.random.fold_in(key, 19), (EXAMPLES * 2,), 0, VOCAB, dtype=jnp.int32)


def shared_head(key):
    base = jax.random.normal(jax.random.fold_in(key, 11), (SEEDS, D, VOCAB), jnp.float32)
    plain = jnp.clip(base, -6.0, 6.0) * (plain_scale / math.sqrt(D))
    chosen = shared_chosen(key)
    strong = jnp.clip(jnp.take(base, chosen, axis=2) * (260.0 / D), -3.0, 3.0)
    return plain.at[:, :, chosen].set(strong)


def shared_targets(key):
    return jax.random.randint(jax.random.fold_in(key, 13), (EXAMPLES, SEQ), 0, VOCAB, dtype=jnp.int32)


def draw_lm_head(key, part):
    return shared_head(key).astype(jnp.bfloat16)


def draw_targets(key, part):
    return shared_targets(key)


def draw_hidden(key, part):
    head = shared_head(key)
    wanted = shared_targets(key)
    chosen = shared_chosen(key)
    stretch = math.sqrt(D) / plain_scale
    along = jnp.take(head, wanted.reshape(-1), axis=2)
    along = jnp.transpose(along, (0, 2, 1)).reshape(SEEDS, EXAMPLES, SEQ, D) * stretch
    along = jnp.clip(along, -4.0, 4.0)
    level = jax.random.uniform(jax.random.fold_in(key, 17), (SEEDS, EXAMPLES, 1, 1), jnp.float32, 0.0, 0.12)
    wobble = jax.random.uniform(jax.random.fold_in(key, 29), (SEEDS, EXAMPLES, SEQ, 1), jnp.float32, 0.6, 1.0)
    strength = level * wobble
    aligned = jnp.take(head, chosen, axis=2)
    aligned = jnp.transpose(aligned, (0, 2, 1)).reshape(SEEDS, EXAMPLES, 2, D) * (math.sqrt(D) / 5.5)
    early = SEQ // 4
    first_spot = jax.random.randint(jax.random.fold_in(key, 31), (SEEDS, EXAMPLES, 1), 0, early, dtype=jnp.int32)
    offset_spot = jax.random.randint(jax.random.fold_in(key, 37), (SEEDS, EXAMPLES, 1), 0, early - 1, dtype=jnp.int32)
    second_spot = (first_spot + 1 + offset_spot) % early
    position = jnp.arange(SEQ, dtype=jnp.int32)[None, None, :]
    first_mask = (position == first_spot)[:, :, :, None]
    second_mask = (position == second_spot)[:, :, :, None]
    noise = jnp.clip(jax.random.normal(jax.random.fold_in(key, 21), (SEEDS, EXAMPLES, SEQ, D), jnp.float32), -5.0, 5.0)
    mixed = noise + strength * along
    mixed = jnp.where(first_mask, aligned[:, :, 0:1, :], mixed)
    mixed = jnp.where(second_mask, aligned[:, :, 1:2, :], mixed)
    return mixed.astype(jnp.bfloat16)


def with_ends(result, stream_key, smallest, high):
    extent = result.shape
    index_at = [jax.random.randint(jax.random.fold_in(stream_key, axis), (), 0, extent[axis]) for axis in range(len(extent))]
    result = result.at[tuple(index_at)].set(smallest)
    longest = extent.index(max(extent))
    index_at[longest] = (index_at[longest] + 1) % extent[longest]
    return result.at[tuple(index_at)].set(high)


def setup_inputs(seed: int = 0) -> dict:
    keys = jax.random.split(jax.random.key(seed), 6)
    hidden = draw_hidden(jax.random.fold_in(keys[5], 71), 0)
    norm_gain = jnp.clip(1.0 + 0.15 * jax.random.normal(keys[1], (SEEDS, D), jnp.float32), 0.25, 1.75)
    lm_head = draw_lm_head(jax.random.fold_in(keys[5], 71), 0)
    targets = draw_targets(jax.random.fold_in(keys[5], 71), 0)
    lengths = with_ends(jax.random.randint(keys[4], (EXAMPLES,), SEQ // 4, SEQ + 1), jax.random.fold_in(keys[4], 1), SEQ // 4, SEQ).astype(jnp.int32)
    return dict(hidden=hidden, norm_gain=norm_gain, lm_head=lm_head, targets=targets, lengths=lengths)


rms_epsilon = 1e-05

def score_example(rows, gain, weight, wanted):
    flat = rows.astype(jnp.float32)
    mean_sq = lax.optimization_barrier(jnp.mean(flat * flat, axis=1, keepdims=True))
    normed = (flat * lax.rsqrt(mean_sq + rms_epsilon) * gain).astype(jnp.bfloat16)
    logits = jnp.dot(normed, weight, preferred_element_type=jnp.float32)
    top_value = lax.optimization_barrier(jnp.max(logits, axis=1, keepdims=True))
    scaled_exp = jnp.exp(logits - top_value)
    probability = scaled_exp / lax.optimization_barrier(jnp.sum(scaled_exp, axis=1, keepdims=True))
    column = jnp.arange(logits.shape[1], dtype=jnp.int32)
    onehot = (column[None, :] == wanted[:, None]).astype(jnp.float32)
    distance = probability - onehot
    return jnp.sqrt(lax.optimization_barrier(jnp.sum(distance * distance, axis=1)))

def reference(hidden, norm_gain, lm_head, targets, lengths):

    def per_seed(member):
        states, gain, weight = member
        return lax.map(lambda pair: score_example(pair[0], gain, weight, pair[1]), (states, targets))
    scores = lax.map(per_seed, (hidden, norm_gain.astype(jnp.float32), lm_head))
    position = jnp.arange(SEQ, dtype=jnp.int32)
    valid = position[None, :] < lengths[:, None]
    token_scores = jnp.where(valid[None, :, :], scores, jnp.float32(0.0))
    example_scores = lax.optimization_barrier(jnp.sum(token_scores, axis=2)) / lengths.astype(jnp.float32)[None, :]
    ensemble = lax.optimization_barrier(jnp.sum(example_scores, axis=0)) / SEEDS
    centered = ensemble - jnp.sum(ensemble) / EXAMPLES
    return (token_scores, ensemble, centered)
```

```python
import functools

import jax
import jax.numpy as jnp
from jax import lax
from jax.experimental import pallas as pl
from jax.experimental.pallas import tpu as pltpu
from jax.sharding import PartitionSpec as P

rms_epsilon = 1e-05
MESH = pl.DeviceIdType.MESH


def line_kernel(
    n, chunk, x_ref, gain_ref, w_ref, tgt_ref, out_ref,
    buf, w_buf, stats, own_sem, w_sem, send_sem, recv_sem, stat_send, stat_recv,
):
    me = lax.axis_index("tensor")
    rows, own = x_ref.shape
    vocab = w_ref.shape[1]
    chunks = rows // chunk
    right = jnp.minimum(me + 1, n - 1)
    left = jnp.maximum(me - 1, 0)

    barrier = pltpu.get_barrier_semaphore()
    for k in range(1, n):
        pl.semaphore_signal(
            barrier, inc=1, device_id={"tensor": lax.rem(me + k, n)}, device_id_type=MESH
        )
    pl.semaphore_wait(barrier, n - 1)

    def span(c):
        return pl.ds(pl.multiple_of(c * chunk, chunk), chunk)

    def hop(src, block, c, way):
        return pltpu.make_async_remote_copy(
            src_ref=src,
            dst_ref=buf.at[block, span(c)],
            send_sem=send_sem.at[way, block, c],
            recv_sem=recv_sem.at[block, c],
            device_id={"tensor": right if way == 0 else left},
            device_id_type=MESH,
        )

    def first(c, carry):
        @pl.when(me < n - 1)
        def _():
            hop(x_ref.at[span(c)], me, c, 0).start()

        @pl.when(me > 0)
        def _():
            hop(x_ref.at[span(c)], me, c, 1).start()

        return carry

    lax.fori_loop(0, chunks, first, 0)
    own_copy = pltpu.make_async_copy(x_ref, buf.at[me], own_sem)
    own_copy.start()
    w_copy = pltpu.make_async_copy(w_ref, w_buf, w_sem)
    w_copy.start()

    def relay(d, c):
        @pl.when(me - d >= 0)
        def _():
            block = jnp.maximum(me - d, 0)
            copy = hop(buf.at[block, span(c)], block, c, 0)
            copy.wait_recv()

            @pl.when(me < n - 1)
            def _():
                copy.start()

        @pl.when(me + d < n)
        def _():
            block = jnp.minimum(me + d, n - 1)
            copy = hop(buf.at[block, span(c)], block, c, 1)
            copy.wait_recv()

            @pl.when(me > 0)
            def _():
                copy.start()

    def middle(i, carry):
        relay(1 + i // chunks, lax.rem(i, chunks))
        return carry

    lax.fori_loop(0, (n - 2) * chunks, middle, 0)
    own_copy.wait()
    w_copy.wait()

    def stat_copy(k, c):
        return pltpu.make_async_remote_copy(
            src_ref=stats.at[me, c],
            dst_ref=stats.at[me, c],
            send_sem=stat_send.at[k, c],
            recv_sem=stat_recv.at[me, c],
            device_id={"tensor": lax.rem(me + k, n)},
            device_id_type=MESH,
        )

    def last(c, carry):
        relay(n - 1, c)
        at = span(c)
        square = jnp.zeros((chunk, 1), jnp.float32)
        for j in range(n):
            part = buf[j, at].astype(jnp.float32)
            square += jnp.sum(part * part, axis=1, keepdims=True)
        scale = lax.rsqrt(square / (own * n) + rms_epsilon)
        logits = jnp.zeros((chunk, vocab), jnp.float32)
        for j in range(n):
            part = buf[j, at].astype(jnp.float32)
            normed = (part * scale * gain_ref[j]).astype(jnp.bfloat16)
            logits += jnp.dot(
                normed, w_buf[pl.ds(j * own, own), :], preferred_element_type=jnp.float32
            )
        top = jnp.max(logits, axis=1, keepdims=True)
        mass = jnp.exp(logits - top)
        column = lax.broadcasted_iota(jnp.int32, (chunk, vocab), 1) + me * vocab
        hit = jnp.where(column == tgt_ref[at, :], mass, 0.0)
        lane = lax.broadcasted_iota(jnp.int32, (chunk, 128), 1)
        packed = jnp.where(
            lane == 0,
            top,
            jnp.where(
                lane == 1,
                jnp.sum(mass, axis=1, keepdims=True),
                jnp.where(
                    lane == 2,
                    jnp.sum(mass * mass, axis=1, keepdims=True),
                    jnp.sum(hit, axis=1, keepdims=True),
                ),
            ),
        )
        stats[me, c] = packed.T[:8]
        for k in range(1, n):
            stat_copy(k, c).start()
        return carry

    lax.fori_loop(0, chunks, last, 0)

    def finish(c, carry):
        for k in range(1, n):
            peer = lax.rem(me + k, n)
            pltpu.make_async_remote_copy(
                src_ref=stats.at[peer, c],
                dst_ref=stats.at[peer, c],
                send_sem=stat_send.at[k, c],
                recv_sem=stat_recv.at[peer, c],
                device_id={"tensor": peer},
                device_id_type=MESH,
            ).wait_recv()
        top = stats[0, c, 0:1]
        for j in range(1, n):
            top = jnp.maximum(top, stats[j, c, 0:1])
        mass = jnp.zeros_like(top)
        square = jnp.zeros_like(top)
        hit = jnp.zeros_like(top)
        for j in range(n):
            factor = jnp.exp(stats[j, c, 0:1] - top)
            mass += stats[j, c, 1:2] * factor
            square += stats[j, c, 2:3] * (factor * factor)
            hit += stats[j, c, 3:4] * factor
        spread = square / (mass * mass) - 2.0 * hit / mass + 1.0
        out_ref[pl.ds(c, 1), :] = jnp.sqrt(jnp.maximum(spread, 0.0))
        return carry

    lax.fori_loop(0, chunks, finish, 0)

    def drain(i, carry):
        block, c = i // chunks, lax.rem(i, chunks)

        @pl.when((me < n - 1) & (block <= me))
        def _():
            hop(buf.at[block, span(c)], block, c, 0).wait_send()

        @pl.when((me > 0) & (block >= me))
        def _():
            hop(buf.at[block, span(c)], block, c, 1).wait_send()

        return carry

    lax.fori_loop(0, n * chunks, drain, 0)

    def drain_stats(c, carry):
        for k in range(1, n):
            stat_copy(k, c).wait_send()
        return carry

    lax.fori_loop(0, chunks, drain_stats, 0)


def row_errors(x, gain, weight, wanted, n):
    rows, own = x.shape
    depth, vocab = weight.shape
    chunk = rows
    while chunk % 256 == 0 and n * (rows // chunk) < 128 and chunk > 128:
        chunk //= 2
    if rows % 128 == 0 and n * (rows // 128) <= 128:
        chunk = 128
    chunks = rows // chunk
    dma = pltpu.SemaphoreType.DMA
    out = pl.pallas_call(
        functools.partial(line_kernel, n, chunk),
        out_shape=jax.ShapeDtypeStruct((chunks, chunk), jnp.float32),
        in_specs=[
            pl.BlockSpec(memory_space=pl.ANY),
            pl.BlockSpec(memory_space=pltpu.VMEM),
            pl.BlockSpec(memory_space=pl.ANY),
            pl.BlockSpec(memory_space=pltpu.VMEM),
        ],
        out_specs=pl.BlockSpec(memory_space=pltpu.VMEM),
        scratch_shapes=[
            pltpu.VMEM((n, rows, own), x.dtype),
            pltpu.VMEM((depth, vocab), weight.dtype),
            pltpu.VMEM((n, chunks, 8, chunk), jnp.float32),
            dma,
            dma,
            dma((2, n, chunks)),
            dma((n, chunks)),
            dma((n, chunks)),
            dma((n, chunks)),
        ],
        compiler_params=pltpu.CompilerParams(
            collective_id=0, has_side_effects=True, vmem_limit_bytes=60 * 1024 * 1024
        ),
        name="line_scores",
    )(x, gain.reshape(n, 1, own), weight, wanted.reshape(rows, 1))
    return out.reshape(rows)


def shards(hidden, norm_gain, lm_head, targets, lengths):
    per_group, seq_len, own_width = (hidden.shape[1], hidden.shape[2], hidden.shape[3])
    row_count = per_group * seq_len
    flat = hidden.reshape(row_count, own_width)
    scores = row_errors(
        flat, norm_gain[0], lm_head[0], targets, lax.axis_size("tensor")
    ).reshape(per_group, seq_len)
    position = jnp.arange(seq_len, dtype=jnp.int32)
    valid = position[None, :] < lengths[:, None]
    token_scores = jnp.where(valid, scores, jnp.float32(0.0))
    example_scores = jnp.sum(token_scores, axis=1) / lengths.astype(jnp.float32)
    members = lax.axis_size("seed")
    groups = lax.axis_size("dp")
    ensemble = lax.psum(example_scores, "seed") / members
    batch_total = lax.psum(jnp.sum(ensemble), "dp")
    centered = ensemble - batch_total / (per_group * groups)
    return (token_scores[None, :, :], ensemble, centered)


def solution(mesh):
    return jax.shard_map(
        shards,
        mesh=mesh,
        in_specs=(
            P("seed", "dp", None, "tensor"),
            P("seed", None),
            P("seed", None, "tensor"),
            P("dp", None),
            P("dp"),
        ),
        out_specs=(P("seed", "dp", None), P("dp"), P("dp")),
        check_vma=False,
    )
```

```python
import functools

import jax
import jax.numpy as jnp
from jax import lax
from jax.experimental import pallas as pl
from jax.experimental.pallas import tpu as pltpu
from jax.sharding import PartitionSpec as P

rms_epsilon = 1e-05
MESH = pl.DeviceIdType.MESH


def line_kernel(
    n, chunk, x_ref, gain_ref, w_ref, tgt_ref, out_ref,
    buf, w_buf, stats, own_sem, w_sem, send_sem, recv_sem, stat_send, stat_recv,
):
    me = lax.axis_index("tensor")
    rows, own = x_ref.shape
    vocab = w_ref.shape[1]
    chunks = rows // chunk
    right = jnp.minimum(me + 1, n - 1)
    left = jnp.maximum(me - 1, 0)

    barrier = pltpu.get_barrier_semaphore()
    for k in range(1, n):
        pl.semaphore_signal(
            barrier, inc=1, device_id={"tensor": lax.rem(me + k, n)}, device_id_type=MESH
        )
    pl.semaphore_wait(barrier, n - 1)

    def span(c):
        return pl.ds(pl.multiple_of(c * chunk, chunk), chunk)

    def hop(src, block, c, way):
        return pltpu.make_async_remote_copy(
            src_ref=src,
            dst_ref=buf.at[block, span(c)],
            send_sem=send_sem.at[way, block, c],
            recv_sem=recv_sem.at[block, c],
            device_id={"tensor": right if way == 0 else left},
            device_id_type=MESH,
        )

    def first(c, carry):
        @pl.when(me < n - 1)
        def _():
            hop(x_ref.at[span(c)], me, c, 0).start()

        @pl.when(me > 0)
        def _():
            hop(x_ref.at[span(c)], me, c, 1).start()

        return carry

    lax.fori_loop(0, chunks, first, 0)
    own_copy = pltpu.make_async_copy(x_ref, buf.at[me], own_sem)
    own_copy.start()
    w_copy = pltpu.make_async_copy(w_ref, w_buf, w_sem)
    w_copy.start()

    def relay(d, c):
        @pl.when(me - d >= 0)
        def _():
            block = jnp.maximum(me - d, 0)
            copy = hop(buf.at[block, span(c)], block, c, 0)
            copy.wait_recv()

            @pl.when(me < n - 1)
            def _():
                copy.start()

        @pl.when(me + d < n)
        def _():
            block = jnp.minimum(me + d, n - 1)
            copy = hop(buf.at[block, span(c)], block, c, 1)
            copy.wait_recv()

            @pl.when(me > 0)
            def _():
                copy.start()

    def middle(i, carry):
        relay(1 + i // chunks, lax.rem(i, chunks))
        return carry

    lax.fori_loop(0, (n - 2) * chunks, middle, 0)
    own_copy.wait()
    w_copy.wait()

    def stat_copy(k, c):
        return pltpu.make_async_remote_copy(
            src_ref=stats.at[me, c],
            dst_ref=stats.at[me, c],
            send_sem=stat_send.at[k, c],
            recv_sem=stat_recv.at[me, c],
            device_id={"tensor": lax.rem(me + k, n)},
            device_id_type=MESH,
        )

    def last(c, carry):
        relay(n - 1, c)
        at = span(c)
        square = jnp.zeros((chunk, 1), jnp.float32)
        for j in range(n):
            part = buf[j, at].astype(jnp.float32)
            square += jnp.sum(part * part, axis=1, keepdims=True)
        scale = lax.rsqrt(square / (own * n) + rms_epsilon)
        logits = jnp.zeros((chunk, vocab), jnp.float32)
        for j in range(n):
            part = buf[j, at].astype(jnp.float32)
            normed = (part * scale * gain_ref[j]).astype(jnp.bfloat16)
            logits += jnp.dot(
                normed, w_buf[pl.ds(j * own, own), :], preferred_element_type=jnp.float32
            )
        top = jnp.max(logits, axis=1, keepdims=True)
        mass = jnp.exp(logits - top)
        column = lax.broadcasted_iota(jnp.int32, (chunk, vocab), 1) + me * vocab
        hit = jnp.where(column == tgt_ref[at, :], mass, 0.0)
        lane = lax.broadcasted_iota(jnp.int32, (chunk, 128), 1)
        packed = jnp.where(
            lane == 0,
            top,
            jnp.where(
                lane == 1,
                jnp.sum(mass, axis=1, keepdims=True),
                jnp.where(
                    lane == 2,
                    jnp.sum(mass * mass, axis=1, keepdims=True),
                    jnp.sum(hit, axis=1, keepdims=True),
                ),
            ),
        )
        stats[me, c] = packed.T[:8]
        for k in range(1, n):
            stat_copy(k, c).start()
        return carry

    lax.fori_loop(0, chunks, last, 0)

    def finish(c, carry):
        for k in range(1, n):
            peer = lax.rem(me + k, n)
            pltpu.make_async_remote_copy(
                src_ref=stats.at[peer, c],
                dst_ref=stats.at[peer, c],
                send_sem=stat_send.at[k, c],
                recv_sem=stat_recv.at[peer, c],
                device_id={"tensor": peer},
                device_id_type=MESH,
            ).wait_recv()
        top = stats[0, c, 0:1]
        for j in range(1, n):
            top = jnp.maximum(top, stats[j, c, 0:1])
        mass = jnp.zeros_like(top)
        square = jnp.zeros_like(top)
        hit = jnp.zeros_like(top)
        for j in range(n):
            factor = jnp.exp(stats[j, c, 0:1] - top)
            mass += stats[j, c, 1:2] * factor
            square += stats[j, c, 2:3] * (factor * factor)
            hit += stats[j, c, 3:4] * factor
        spread = square / (mass * mass) - 2.0 * hit / mass + 1.0
        out_ref[pl.ds(c, 1), :] = jnp.sqrt(jnp.maximum(spread, 0.0))
        return carry

    lax.fori_loop(0, chunks, finish, 0)

    def drain(i, carry):
        block, c = i // chunks, lax.rem(i, chunks)

        @pl.when((me < n - 1) & (block <= me))
        def _():
            hop(buf.at[block, span(c)], block, c, 0).wait_send()

        @pl.when((me > 0) & (block >= me))
        def _():
            hop(buf.at[block, span(c)], block, c, 1).wait_send()

        return carry

    lax.fori_loop(0, n * chunks, drain, 0)

    def drain_stats(c, carry):
        for k in range(1, n):
            stat_copy(k, c).wait_send()
        return carry

    lax.fori_loop(0, chunks, drain_stats, 0)


def row_errors(x, gain, weight, wanted, n):
    rows, own = x.shape
    depth, vocab = weight.shape
    chunk = rows
    while chunk % 256 == 0 and n * (rows // chunk) < 128 and chunk > 128:
        chunk //= 2
    if rows % 128 == 0 and n * (rows // 128) <= 128:
        chunk = 128
    chunks = rows // chunk
    dma = pltpu.SemaphoreType.DMA
    out = pl.pallas_call(
        functools.partial(line_kernel, n, chunk),
        out_shape=jax.ShapeDtypeStruct((chunks, chunk), jnp.float32),
        in_specs=[
            pl.BlockSpec(memory_space=pl.ANY),
            pl.BlockSpec(memory_space=pltpu.VMEM),
            pl.BlockSpec(memory_space=pl.ANY),
            pl.BlockSpec(memory_space=pltpu.VMEM),
        ],
        out_specs=pl.BlockSpec(memory_space=pltpu.VMEM),
        scratch_shapes=[
            pltpu.VMEM((n, rows, own), x.dtype),
            pltpu.VMEM((depth, vocab), weight.dtype),
            pltpu.VMEM((n, chunks, 8, chunk), jnp.float32),
            dma,
            dma,
            dma((2, n, chunks)),
            dma((n, chunks)),
            dma((n, chunks)),
            dma((n, chunks)),
        ],
        compiler_params=pltpu.CompilerParams(
            collective_id=0, has_side_effects=True, vmem_limit_bytes=60 * 1024 * 1024
        ),
        name="line_scores",
    )(x, gain.reshape(n, 1, own), weight, wanted.reshape(rows, 1))
    return out.reshape(rows)


def totals_kernel(members, groups, per_group, mine_ref, out_ref, parts, send_sem, recv_sem):
    seed, group = lax.axis_index("seed"), lax.axis_index("dp")
    count = members * groups
    me = seed * groups + group

    def device(peer):
        return {"seed": peer // groups, "dp": lax.rem(peer, groups)}

    barrier = pltpu.get_barrier_semaphore()
    for k in range(1, count):
        pl.semaphore_signal(
            barrier, inc=1, device_id=device(lax.rem(me + k, count)), device_id_type=MESH
        )
    pl.semaphore_wait(barrier, count - 1)

    def part(k, slot):
        return pltpu.make_async_remote_copy(
            src_ref=mine_ref,
            dst_ref=parts.at[slot],
            send_sem=send_sem.at[k],
            recv_sem=recv_sem.at[slot],
            device_id=device(lax.rem(me + k, count)),
            device_id_type=MESH,
        )

    for k in range(1, count):
        part(k, me).start()
    for k in range(1, count):
        part(k, lax.rem(me + k, count)).wait_recv()
    whole = mine_ref[...]
    for k in range(1, count):
        whole += parts[lax.rem(me + k, count)]
    ensemble = mine_ref[...]
    for k in range(1, members):
        ensemble += parts[lax.rem(seed + k, members) * groups + group]
    ensemble = ensemble / members
    total = jnp.sum(whole, keepdims=True) / members
    out_ref[0] = ensemble
    out_ref[1] = ensemble - total / (per_group * groups)
    for k in range(1, count):
        part(k, me).wait_send()


def group_totals(example_scores, members, groups):
    per_group = example_scores.shape[0]
    count = members * groups
    width = -(-per_group // 128) * 128
    padded = jnp.pad(example_scores[None, :], ((0, 7), (0, width - per_group)))
    out = pl.pallas_call(
        functools.partial(totals_kernel, members, groups, per_group),
        out_shape=jax.ShapeDtypeStruct((2, 8, width), jnp.float32),
        in_specs=[pl.BlockSpec(memory_space=pltpu.VMEM)],
        out_specs=pl.BlockSpec(memory_space=pltpu.VMEM),
        scratch_shapes=[
            pltpu.VMEM((count, 8, width), jnp.float32),
            pltpu.SemaphoreType.DMA((count,)),
            pltpu.SemaphoreType.DMA((count,)),
        ],
        compiler_params=pltpu.CompilerParams(collective_id=1, has_side_effects=True),
        name="group_totals",
    )(padded)
    return out[0, 0, :per_group], out[1, 0, :per_group]


def shards(hidden, norm_gain, lm_head, targets, lengths):
    per_group, seq_len, own_width = (hidden.shape[1], hidden.shape[2], hidden.shape[3])
    row_count = per_group * seq_len
    flat = hidden.reshape(row_count, own_width)
    scores = row_errors(
        flat, norm_gain[0], lm_head[0], targets, lax.axis_size("tensor")
    ).reshape(per_group, seq_len)
    position = jnp.arange(seq_len, dtype=jnp.int32)
    valid = position[None, :] < lengths[:, None]
    token_scores = jnp.where(valid, scores, jnp.float32(0.0))
    example_scores = jnp.sum(token_scores, axis=1) / lengths.astype(jnp.float32)
    ensemble, centered = group_totals(
        example_scores, lax.axis_size("seed"), lax.axis_size("dp")
    )
    return (token_scores[None, :, :], ensemble, centered)


def solution(mesh):
    return jax.shard_map(
        shards,
        mesh=mesh,
        in_specs=(
            P("seed", "dp", None, "tensor"),
            P("seed", None),
            P("seed", None, "tensor"),
            P("dp", None),
            P("dp"),
        ),
        out_specs=(P("seed", "dp", None), P("dp"), P("dp")),
        check_vma=False,
    )
```
